32 devices in a mesh: layer: 4 (over y, core), slab: 8 (over z, x).
Axes of the slice: x: 2, y: 2, z: 4, core: 2. Of those that a mesh axis runs over, the one named last changes fastest.
Arguments:
- weights: bfloat16 [8192, 16384], P('slab', 'layer'), may hold values from -0.29882812 to 0.29882812
- whitening: bfloat16 [8192, 8192], P('slab'), may hold values from -1 to 10, as said below
- test_matrix: int32 [16384, 1024], P(('layer', 'slab')), may hold values from -4 to 4
Outputs:
- basis: float32 [8192, 1024], P('slab')
- coefficients: float32 [16384, 1024], P('layer', 'slab')
The draws below stay inside these ranges and needn't reach their ends.
Inputs may be any that keep to these rules, and one draw needn't show every extreme that they name: whitening is lower triangular with diagonal entries between 1 and 10.
All inputs are finite; a program needn't handle non-finite values.
Results may differ from the reference program's by a relative error of at most 0.006.
Values may be sent and summed in bfloat16 or wider, within the bound.
A program may use at most 128 MiB of HBM per device.

```python
import math
import jax
import jax.numpy as jnp
from jax import lax

D = 8192
RANK = 1024
COLS = 16384


def draw_whitening(key, part):
    key_off = jax.random.fold_in(key, 11)
    key_diag = jax.random.fold_in(key, 12)
    row_index = jnp.arange(D)[:, None]
    col_index = jnp.arange(D)[None, :]
    spread = 0.5 / math.sqrt(D)
    below = jnp.clip(jax.random.normal(key_off, (D, D)), -4.0, 4.0) * spread
    diagonal = jnp.exp(jax.random.uniform(key_diag, (D,), minval=0.0, maxval=math.log(10.0)))
    result = jnp.where(col_index < row_index, below, 0.0) + jnp.diag(diagonal)
    return result.astype(jnp.float32).astype(jnp.bfloat16)


def set_ends(drawn, stream_key, smallest, high):
    longest = drawn.shape.index(max(drawn.shape))
    spots = []
    for shift in (0, 1):
        where = [jax.random.randint(jax.random.fold_in(stream_key, axis), (), 0, length) for axis, length in enumerate(drawn.shape)]
        where[longest] = (where[longest] + shift) % drawn.shape[longest]
        spots.append(tuple(where))
    return drawn.at[spots[0]].set(smallest).at[spots[1]].set(high)


def block_levels(rng, shape, cuts, smallest, largest):
    level = 1.0
    for dim, parts in cuts:
        steps = jax.random.uniform(jax.random.fold_in(jax.random.fold_in(rng, 6), dim), (parts,), jnp.float32, smallest / len(cuts), largest / len(cuts))
        level = level * jnp.repeat(jnp.exp(steps), shape[dim] // parts).reshape((-1,) + (1,) * (len(shape) - 1 - dim))
    return level


def noise(stream_key, shape, width, most, cuts=(), held_as=jnp.bfloat16):
    entries = jax.random.normal(stream_key, shape, jnp.float32) * width
    if len(cuts) > 0:
        entries = block_levels(stream_key, shape, cuts, -0.22, 0.18) * entries
    return jnp.clip(entries, min=-most, max=most).astype(held_as)


def setup_inputs(seed: int = 0) -> dict:
    key_list = jax.random.split(jax.random.key(seed), 4)
    weights = noise(key_list[0], (D, COLS), 0.05, 0.29882812, ((0, 8), (1, 4)))
    whitening = draw_whitening(jax.random.fold_in(key_list[3], 71), 0)
    test_matrix = set_ends(jax.random.randint(key_list[2], (COLS, RANK), -4, 5), jax.random.fold_in(key_list[2], 1), -4, 4).astype(jnp.int32)
    return {"weights": weights, "whitening": whitening, "test_matrix": test_matrix}


def reference(weights, whitening, test_matrix):
    test_values = test_matrix.astype(jnp.bfloat16)
    sketch = jnp.dot(weights.astype(jnp.float32), test_values.astype(jnp.float32), preferred_element_type=jnp.float32).astype(jnp.bfloat16)
    whitened = jnp.dot(whitening.astype(jnp.float32), sketch.astype(jnp.float32), preferred_element_type=jnp.float32)
    gram_matrix = jnp.dot(whitened.T.astype(jnp.float32), whitened.astype(jnp.float32), precision=lax.Precision.HIGHEST, preferred_element_type=jnp.float32)
    factor = jnp.linalg.cholesky(gram_matrix)
    ortho = jax.scipy.linalg.solve_triangular(factor, whitened.T, lower=True).T
    basis_half = ortho.astype(jnp.bfloat16)
    basis = basis_half.astype(jnp.float32) * math.sqrt(D)
    projected = jnp.dot(whitening.T.astype(jnp.float32), basis_half.astype(jnp.float32), preferred_element_type=jnp.float32).astype(jnp.bfloat16)
    coefficients = jnp.dot(weights.T.astype(jnp.float32), projected.astype(jnp.float32), preferred_element_type=jnp.float32)
    return (basis, coefficients)
```

```python
import functools
import math

import jax
import jax.numpy as jnp
from jax import lax
from jax.experimental import pallas as pl
from jax.experimental.pallas import tpu as pltpu
from jax.sharding import PartitionSpec as P

BLOCK = 128
PANEL = 32
GROUP = 8
HIGHEST = lax.Precision.HIGHEST


def inverse_factor_kernel(size, panel, block_ref, inverse_ref, work):
    rows = lax.broadcasted_iota(jnp.int32, (size, size), 0)
    lanes = lax.broadcasted_iota(jnp.int32, (size, size), 1)
    work[:, :size] = block_ref[...]
    work[:, size:] = (rows == lanes).astype(jnp.float32)
    place = lax.broadcasted_iota(jnp.int32, (panel, size), 0)
    for start in range(0, size, panel):
        halves = [work[start : start + panel, :size], work[start : start + panel, size:]]
        for group in range(0, panel, GROUP):
            spread = [
                jnp.broadcast_to(
                    halves[0][:, start + group + k : start + group + k + 1], (panel, size)
                )
                for k in range(GROUP)
            ]
            for k in range(GROUP):
                step = group + k
                scale = lax.rsqrt(spread[k][step : step + 1, :])
                factor = spread[k] * scale
                for later in range(k + 1, GROUP):
                    pivot = spread[later][step : step + 1, :] * scale
                    spread[later] = spread[later] - factor * pivot
                for i in range(2):
                    pivot_row = halves[i][step : step + 1, :] * scale
                    cleared = halves[i] - factor * pivot_row
                    halves[i] = jnp.where(
                        place == step, pivot_row, jnp.where(place > step, cleared, halves[i])
                    )
        inverse_ref[start : start + panel, :] = halves[1]
        if start + panel < size:
            for i in range(2):
                update = lax.dot_general(
                    halves[0],
                    halves[i],
                    (((0,), (0,)), ((), ())),
                    precision=HIGHEST,
                    preferred_element_type=jnp.float32,
                )
                half = slice(i * size, (i + 1) * size)
                work[start + panel :, half] = (
                    work[start + panel :, half] - update[start + panel :, :]
                )


def inverse_factor(stacked, size):
    corner = pl.BlockSpec((size, size), lambda i: (0, 0))
    return pl.pallas_call(
        functools.partial(inverse_factor_kernel, size, PANEL),
        grid=(1,),
        out_shape=jax.ShapeDtypeStruct((size, size), jnp.float32),
        in_specs=[corner],
        out_specs=corner,
        scratch_shapes=[pltpu.VMEM((size, 2 * size), jnp.float32)],
        name="inverse_factor",
    )(stacked)


def times_transposed(left, right):
    return lax.dot_general(
        left,
        right,
        (((1,), (1,)), ((), ())),
        precision=HIGHEST,
        preferred_element_type=jnp.float32,
    )


def orthogonal(gram_matrix, whitened):
    rank = gram_matrix.shape[0]
    block = min(BLOCK, rank)
    stacked = jnp.concatenate([gram_matrix, whitened], axis=0)
    solved = []
    for start in range(0, rank, block):
        rest = rank - start - block
        inverse = inverse_factor(stacked, block)
        panel = times_transposed(stacked[block:, :block], inverse)
        solved.append(panel[rest:])
        if rest > 0:
            stacked = stacked[block:, block:] - times_transposed(panel, panel[:rest])
    return jnp.concatenate(solved, axis=1)


def on_device(weights, whitening, test_matrix):
    rank_width = test_matrix.shape[1]
    slice_width = rank_width // lax.axis_size("layer")
    test_values = test_matrix.astype(jnp.bfloat16)
    sketch_terms = jnp.dot(
        weights,
        lax.all_gather(test_values, "slab", axis=0, tiled=True),
        preferred_element_type=jnp.float32,
    )
    sketch = lax.psum_scatter(sketch_terms, "layer", scatter_dimension=1, tiled=True).astype(
        jnp.bfloat16
    )
    whitened_part = jnp.dot(
        whitening,
        lax.all_gather(sketch, "slab", axis=0, tiled=True),
        preferred_element_type=jnp.float32,
    )
    whitened = lax.all_gather(whitened_part, "layer", axis=1, tiled=True)
    local_gram = lax.dot_general(
        whitened_part,
        whitened,
        (((0,), (0,)), ((), ())),
        precision=HIGHEST,
        preferred_element_type=jnp.float32,
    )
    gram_matrix = lax.all_gather(
        lax.psum(local_gram, "slab"), "layer", axis=0, tiled=True
    )
    ortho = orthogonal(gram_matrix, whitened)
    basis_half = ortho.astype(jnp.bfloat16)
    basis = basis_half.astype(jnp.float32) * math.sqrt(whitening.shape[1])
    own_slice = lax.dynamic_slice_in_dim(
        basis_half, lax.axis_index("layer") * slice_width, slice_width, 1
    )
    projected_part = lax.psum_scatter(
        lax.dot_general(
            whitening, own_slice, (((0,), (0,)), ((), ())), preferred_element_type=jnp.float32
        ).astype(jnp.bfloat16),
        "slab",
        scatter_dimension=0,
        tiled=True,
    )
    projected = lax.all_gather(projected_part, "layer", axis=1, tiled=True)
    coefficients = lax.psum_scatter(
        lax.dot_general(
            weights, projected, (((0,), (0,)), ((), ())), preferred_element_type=jnp.float32
        ).astype(jnp.bfloat16),
        "slab",
        scatter_dimension=1,
        tiled=True,
    ).astype(jnp.float32)
    return (basis, coefficients)


def solution(mesh):
    placed = (P("slab", "layer"), P("slab", None), P(("layer", "slab"), None))
    return jax.shard_map(
        on_device,
        mesh=mesh,
        in_specs=placed,
        out_specs=(P("slab", None), P("layer", "slab")),
        check_vma=False,
    )
```
